32 devices in a mesh: gx: 4 (over y, core), gy: 8 (over z, x).
Axes of the slice: x: 2, y: 2, z: 4, core: 2. Of those that a mesh axis runs over, the one named last changes fastest.
Arguments:
- species: float32 [9, 32, 64, 128], P(None, 'gx', 'gy'), may hold values from -4 to 4
- flow_fields: float32 [5, 32, 64, 128], P(None, 'gx', 'gy'), may hold values from -5 to 5
- classes: int32 [32, 64], P('gx', 'gy'), may hold values from 1 to 4, as said below
- diffusivity: float32 [14], replicated, may hold values from 0.2 to 0.6
- left_form: float32 [19, 9], replicated, may hold values from -2 to 2
- right_form: float32 [19, 9], replicated, may hold values from -2 to 2
- stoich: float32 [19, 9], replicated, may hold values from -1.25 to 1.25
- heat_release: float32 [19], replicated, may hold values from -3 to 3
- arrhenius_prefactor: float32 [19], replicated, may hold values from 0.4 to 4
- arrhenius_energy: float32 [19], replicated, may hold values from 0.5 to 2
- newton_matrix: float32 [10, 10], replicated, may hold values from -0.5 to 1.5
Outputs:
- species_out: float32 [9, 32, 64, 128], P(None, 'gx', 'gy')
- flow_out: float32 [5, 32, 64, 128], P(None, 'gx', 'gy')
The draws below stay inside these ranges and needn't reach their ends.
Inputs may be any that keep to these rules, and one draw needn't show every extreme that they name: `classes`: 1 where a column takes one substep, 2 to 4 otherwise. Among the columns of one device at most 32 have a class over 1, and some device has exactly that many; two devices with the same gx index whose gy indices differ by half the gy axis hold at most 40 such columns together, and some pair has exactly that many.
All inputs are finite; a program needn't handle non-finite values.
Results may differ from the reference program's by a relative error of at most 0.0003.
Values sent between devices are 32-bit elements; how exact they have to be, the bound alone decides.
A program may use at most 64 MiB of HBM per device.

```python
import math
import jax
import jax.numpy as jnp
from jax import lax

NSPEC = 9
NREAC = 19
FLOW = 5
CX = 8
CY = 8
NZ = 128
NFIELD = 14
NX = 32
NY = 64


def draw_classes(key, part):
    blocks_x = NX // CX
    blocks_y = NY // CY
    half_axis = blocks_y // 2
    columns = CX * CY
    stiff_cap = columns // 2
    pairing_limit = 5 * columns // 8
    subkeys = jax.random.split(key, 6)
    flagged = jax.random.randint(subkeys[0], (blocks_x, half_axis), 0, 2)
    forcing_applied = jax.random.randint(subkeys[1], (), 0, blocks_x * half_axis)
    chosen_pair = (jnp.arange(blocks_x * half_axis).reshape(blocks_x, half_axis) == forcing_applied).astype(jnp.int32)
    flagged = jnp.maximum(flagged, chosen_pair)
    heavy_left = jax.random.randint(subkeys[2], (blocks_x, half_axis), 0, 2)
    quiet_count = jax.random.randint(subkeys[3], (blocks_x, blocks_y), columns // 16, columns // 8 + 1)
    front_left = jnp.where(heavy_left == 1, stiff_cap, pairing_limit - stiff_cap)
    leading_east_neighbour = pairing_limit - front_left
    left_count = jnp.where(flagged == 1, front_left, quiet_count[:, :half_axis])
    right_count = jnp.where(flagged == 1, leading_east_neighbour, quiet_count[:, half_axis:])
    counts = jnp.concatenate([left_count, right_count], axis=1)
    scores = jax.random.randint(subkeys[4], (blocks_x, blocks_y, columns), 0, 1 << 20) * columns + jnp.arange(columns)
    rank_order = jnp.argsort(jnp.argsort(scores, axis=-1, stable=True), axis=-1, stable=True)
    levels = jax.random.randint(subkeys[5], (blocks_x, blocks_y, columns), 2, 5)
    marked = jnp.where(rank_order < counts[..., None], levels, 1)
    class_grid = marked.reshape(blocks_x, blocks_y, CX, CY).transpose(0, 2, 1, 3).reshape(NX, NY)
    return class_grid.astype(jnp.int32)


def draw_newton_matrix(key, part):
    components = NSPEC + 1
    spread = jnp.clip(jax.random.normal(key, (components, components), jnp.float32), -4.0, 4.0) * 0.12
    return jnp.eye(components, dtype=jnp.float32) + spread


def block_scale(key, dims, shards, least, high):
    loudness = 1.0
    for axis_at, shards_of in shards:
        draws = jax.random.uniform(jax.random.fold_in(jax.random.fold_in(key, 6), axis_at), (shards_of,), jnp.float32, least / len(shards), high / len(shards))
        loudness = loudness * jnp.repeat(jnp.exp(draws), dims[axis_at] // shards_of).reshape((-1,) + (1,) * (len(dims) - 1 - axis_at))
    return loudness


def noise(rng, extent, scale, limit, cuts=(), kind=jnp.bfloat16):
    level = block_scale(rng, extent, cuts, -0.22, 0.18) if cuts else 1.0
    drawn = jax.random.normal(rng, extent, jnp.float32) * scale * level
    return jnp.minimum(jnp.maximum(drawn, -limit), limit).astype(kind)


def setup_inputs(seed: int = 0) -> dict:
    keys = jax.random.split(jax.random.key(seed), 12)
    species = noise(keys[0], (NSPEC, NX, NY, NZ), 0.7, 4.0, ((1, 4), (2, 8)), jnp.float32)
    flow_fields = noise(keys[1], (FLOW, NX, NY, NZ), 1.0, 5.0, ((1, 4), (2, 8)), jnp.float32)
    classes = draw_classes(jax.random.fold_in(keys[11], 71), 0)
    diffusivity = jnp.clip(jnp.exp(jax.random.uniform(keys[3], (NFIELD,), jnp.float32, math.log(0.2), math.log(0.6))), 0.2, 0.6)
    left_form = noise(keys[4], (NREAC, NSPEC), NSPEC ** -0.5, 2.0, (), jnp.float32)
    right_form = noise(keys[5], (NREAC, NSPEC), NSPEC ** -0.5, 2.0, (), jnp.float32)
    stoich = noise(keys[6], (NREAC, NSPEC), NREAC ** -0.5, 1.25, (), jnp.float32)
    heat_release = noise(keys[7], (NREAC,), 0.3, 3.0, (), jnp.float32)
    arrhenius_prefactor = jnp.clip(jnp.exp(jax.random.uniform(keys[8], (NREAC,), jnp.float32, math.log(0.4), math.log(4.0))), 0.4, 4.0)
    arrhenius_energy = jnp.clip(jax.random.uniform(keys[9], (NREAC,), jnp.float32, 0.5, 2.0), 0.5, 2.0)
    newton_matrix = draw_newton_matrix(jax.random.fold_in(keys[11], 71), 0)
    return {"species": species, "flow_fields": flow_fields, "classes": classes, "diffusivity": diffusivity, "left_form": left_form, "right_form": right_form, "stoich": stoich, "heat_release": heat_release, "arrhenius_prefactor": arrhenius_prefactor, "arrhenius_energy": arrhenius_energy, "newton_matrix": newton_matrix}


TIME_STEP = 0.25
PRECISE = lax.Precision.HIGHEST


def reaction_rates(burning_mixture_status, params):
    left_form, right_form, stoich, heat_release, arrhenius_prefactor, arrhenius_energy = params
    fractions = burning_mixture_status[:-1]
    thermal_kelvin_field = burning_mixture_status[-1]
    left_sum = jnp.tanh(jnp.einsum("rs,scn->rcn", left_form, fractions, precision=PRECISE))
    right_sum = jnp.tanh(jnp.einsum("rs,scn->rcn", right_form, fractions, precision=PRECISE))
    flow_speed_norm = arrhenius_prefactor[:, None, None] * jax.nn.sigmoid(arrhenius_energy[:, None, None] * thermal_kelvin_field[None])
    progress = flow_speed_norm * left_sum * right_sum
    species_rate = jnp.einsum("rs,rcn->scn", stoich, progress, precision=PRECISE)
    heat_rate = jnp.einsum("r,rcn->cn", heat_release, progress, precision=PRECISE)
    return jnp.concatenate([species_rate, heat_rate[None]], axis=0)


def substep(start, step_size, newton_matrix, params):
    current = start
    for repeat in range(3):
        residue = current - start - step_size[None] * reaction_rates(current, params)
        current = current - jnp.einsum("ij,jcn->icn", newton_matrix, residue, precision=PRECISE)
    return current


def wave_line(length):
    waves = 2.0 * jnp.pi * jnp.fft.fftfreq(length)
    return jnp.where(jnp.arange(length) == length // 2, 0.0, waves)


def reference(species, flow_fields, classes, diffusivity, left_form, right_form, stoich, heat_release, arrhenius_prefactor, arrhenius_energy, newton_matrix):
    params = (left_form, right_form, stoich, heat_release, arrhenius_prefactor, arrhenius_energy)
    nspec = species.shape[0]
    fields = jnp.concatenate([species, flow_fields], axis=0)
    stream_vel = flow_fields[1]
    span_vel = flow_fields[2]
    depth_vel = flow_fields[3]

    def transport(pieces):
        field, coefficient = pieces
        ahead_x = jnp.roll(field, -1, 0)
        behind_x = jnp.roll(field, 1, 0)
        ahead_y = jnp.roll(field, -1, 1)
        behind_y = jnp.roll(field, 1, 1)
        ahead_z = jnp.roll(field, -1, 2)
        behind_z = jnp.roll(field, 1, 2)
        laplace_sum = ahead_x + behind_x + ahead_y + behind_y + ahead_z + behind_z - 6.0 * field
        advection = 0.5 * (stream_vel * (ahead_x - behind_x) + span_vel * (ahead_y - behind_y) + depth_vel * (ahead_z - behind_z))
        return field + TIME_STEP * (coefficient * laplace_sum - advection)

    transported = lax.map(transport, (fields, diffusivity))
    burning_mixture_status = jnp.concatenate([transported[:nspec], transported[nspec + 4:nspec + 5]], axis=0)

    def react_row(pieces):
        row_state, row_class = pieces
        class_value = row_class.astype(jnp.float32)
        step_size = (TIME_STEP / class_value)[:, None]
        current = substep(row_state, step_size, newton_matrix, params)
        for section in (1, 2, 3):
            active = (class_value > section)[None, :, None]
            current = jnp.where(active, substep(current, step_size, newton_matrix, params), current)
        return current

    reacted = jnp.moveaxis(lax.map(react_row, (jnp.moveaxis(burning_mixture_status, 1, 0), classes)), 0, 1)
    source = (reacted[nspec] - transported[nspec + 4]) / TIME_STEP
    velocity = transported[nspec + 1:nspec + 4]
    vel_hat = jnp.fft.fftn(velocity, axes=(1, 2, 3))
    source_hat = jnp.fft.fftn(source)
    wave_x = wave_line(NX).reshape(-1, 1, 1)
    wave_y = wave_line(NY).reshape(1, -1, 1)
    wave_z = wave_line(NZ).reshape(1, 1, -1)
    wavenumber_squared = wave_x * wave_x + wave_y * wave_y + wave_z * wave_z
    denom = jnp.where(wavenumber_squared > 0, wavenumber_squared, 1.0)
    dotted = wave_x * vel_hat[0] + wave_y * vel_hat[1] + wave_z * vel_hat[2]
    waves = (wave_x, wave_y, wave_z)
    projected_hat = jnp.stack([vel_hat[axis] - waves[axis] * dotted / denom - 1j * waves[axis] * source_hat / denom for axis in range(3)])
    projected = jnp.real(jnp.fft.ifftn(projected_hat, axes=(1, 2, 3))).astype(jnp.float32)
    species_out = reacted[:nspec]
    flow_out = jnp.concatenate([transported[nspec:nspec + 1], projected, reacted[nspec:nspec + 1]], axis=0)
    return (species_out, flow_out)
```

```python
import functools

import jax
import jax.numpy as jnp
import ml_dtypes
import numpy as np
from jax import lax
from jax.experimental import pallas as pl
from jax.experimental.pallas import tpu as pltpu
from jax.sharding import PartitionSpec as P

TIME_STEP = 0.25
PRECISE = lax.Precision.HIGHEST


def extended(value, sides, width):
    for axis, dim in sides:
        size, length = (lax.axis_size(axis), value.shape[dim])
        up = [(i, (i + 1) % size) for i in range(size)]
        down = [(j, i) for i, j in up]
        last = lax.slice_in_dim(value, length - width, length, axis=dim)
        first = lax.slice_in_dim(value, 0, width, axis=dim)
        before = lax.ppermute(last, axis, up)
        after = lax.ppermute(first, axis, down)
        value = jnp.concatenate([before, value, after], axis=dim)
    return value


def reaction_rates(burning_mixture_status, params):
    left_form, right_form, stoich, heat_release, arrhenius_prefactor, arrhenius_energy = params
    fractions = burning_mixture_status[:-1]
    thermal_kelvin_field = burning_mixture_status[-1]
    left_sum = jnp.tanh(jnp.einsum("rs,scn->rcn", left_form, fractions, precision=PRECISE))
    right_sum = jnp.tanh(jnp.einsum("rs,scn->rcn", right_form, fractions, precision=PRECISE))
    flow_speed_norm = arrhenius_prefactor[:, None, None] * jax.nn.sigmoid(
        arrhenius_energy[:, None, None] * thermal_kelvin_field[None]
    )
    progress = flow_speed_norm * left_sum * right_sum
    species_rate = jnp.einsum("rs,rcn->scn", stoich, progress, precision=PRECISE)
    heat_rate = jnp.einsum("r,rcn->cn", heat_release, progress, precision=PRECISE)
    return jnp.concatenate([species_rate, heat_rate[None]], axis=0)


def substep(start, step_size, newton_matrix, params):
    current = start
    for repeat in range(3):
        residue = current - start - step_size[None] * reaction_rates(current, params)
        current = current - jnp.einsum("ij,jcn->icn", newton_matrix, residue, precision=PRECISE)
    return current


def extras(buffer, class_value, newton_matrix, params):
    step_size = (TIME_STEP / class_value)[:, None]
    for section in (1, 2, 3):
        active = (class_value > section)[None, :, None]
        buffer = jnp.where(active, substep(buffer, step_size, newton_matrix, params), buffer)
    return buffer


def tables(length):
    index = jnp.arange(length, dtype=jnp.int32)
    phase = index[:, None] * index[None, :] % length
    angle = phase.astype(jnp.float32) * (2.0 * jnp.pi / length)
    return (jnp.cos(angle), jnp.sin(angle))


def half_angles(length):
    index = jnp.arange(length, dtype=jnp.int32)
    modes = jnp.arange(length // 2, dtype=jnp.int32)
    phase = index[:, None] * modes[None, :] % length
    angle = phase.astype(jnp.float32) * (2.0 * jnp.pi / length)
    alternate = jnp.where(index % 2 == 0, 1.0, -1.0).astype(jnp.float32)
    return (angle, alternate, modes)


def transform_dim(array, dimension, lookup):
    moved_last = jnp.moveaxis(array, dimension, -1)
    result = jnp.einsum("...j,jk->...k", moved_last, lookup, precision=PRECISE)
    return jnp.moveaxis(result, -1, dimension)


def forward(spectra, dimension):
    length = spectra.shape[dimension]
    cosine, sine_table = tables(length)
    real_part = spectra[:, 0]
    imag_part = spectra[:, 1]
    inner = dimension - 1
    new_real = transform_dim(real_part, inner, cosine) + transform_dim(imag_part, inner, sine_table)
    new_imag = transform_dim(imag_part, inner, cosine) - transform_dim(real_part, inner, sine_table)
    return jnp.stack([new_real, new_imag], axis=1)


def backward(spectra, dimension):
    length = spectra.shape[dimension]
    cosine, sine_table = tables(length)
    real_part = spectra[:, 0]
    imag_part = spectra[:, 1]
    inner = dimension - 1
    new_real = (
        transform_dim(real_part, inner, cosine) - transform_dim(imag_part, inner, sine_table)
    ) / length
    new_imag = (
        transform_dim(imag_part, inner, cosine) + transform_dim(real_part, inner, sine_table)
    ) / length
    return jnp.stack([new_real, new_imag], axis=1)


def forward_packed(values):
    length = values.shape[3]
    angle, alternate, modes = half_angles(length)
    cosine = jnp.cos(angle)
    packed_sine = jnp.where(modes[None, :] == 0, -alternate[:, None], jnp.sin(angle))
    return jnp.stack(
        [transform_dim(values, 3, cosine), -transform_dim(values, 3, packed_sine)], axis=1
    )


def backward_packed(spectra):
    length = 2 * spectra.shape[4]
    angle, alternate, modes = half_angles(length)
    weight = jnp.where(modes == 0, 1.0, 2.0).astype(jnp.float32)
    cos_back = weight[:, None] * jnp.cos(angle.T)
    sin_back = jnp.where(modes[:, None] == 0, -alternate[None, :], 2.0 * jnp.sin(angle.T))
    return (
        transform_dim(spectra[:, 0], 3, cos_back) - transform_dim(spectra[:, 1], 3, sin_back)
    ) / length


def wave_numbers(index, length):
    signed = jnp.where(index < (length + 1) // 2, index, index - length)
    waves = signed.astype(jnp.float32) * (2.0 * jnp.pi / length)
    return jnp.where(index == length // 2, 0.0, waves)


def project(spectra, rows_x, total_x, rows_y, total_y, rows_z, total_z):
    wave_x = wave_numbers(rows_x, total_x)[:, None, None]
    wave_y = wave_numbers(rows_y, total_y)[None, :, None]
    wave_z = wave_numbers(rows_z, total_z)[None, None, :]
    wavenumber_squared = wave_x * wave_x + wave_y * wave_y + wave_z * wave_z
    denom = jnp.where(wavenumber_squared > 0, wavenumber_squared, 1.0)
    vel_real = spectra[:3, 0]
    vel_imag = spectra[:3, 1]
    source_real = spectra[3, 0]
    source_imag = spectra[3, 1]
    inner_product_real = wave_x * vel_real[0] + wave_y * vel_real[1] + wave_z * vel_real[2]
    imaginary_inner_sum = wave_x * vel_imag[0] + wave_y * vel_imag[1] + wave_z * vel_imag[2]
    waves = (wave_x, wave_y, wave_z)
    outputs = []
    for axis in range(3):
        out_real = (
            vel_real[axis]
            - waves[axis] * inner_product_real / denom
            + waves[axis] * source_imag / denom
        )
        out_imag = (
            vel_imag[axis]
            - waves[axis] * imaginary_inner_sum / denom
            - waves[axis] * source_real / denom
        )
        outputs.append(jnp.stack([out_real, out_imag], axis=0))
    return jnp.stack(outputs, axis=0)


def stream_lines(spectra):
    return forward(spectra, 2)


def span_lines(spectra):
    return forward(spectra, 3)


def stream_inverse(spectra):
    return backward(spectra, 2)


def shards(
    species,
    flow_fields,
    classes,
    diffusivity,
    left_form,
    right_form,
    stoich,
    heat_release,
    arrhenius_prefactor,
    arrhenius_energy,
    newton_matrix,
):
    params = (left_form, right_form, stoich, heat_release, arrhenius_prefactor, arrhenius_energy)
    nspec = species.shape[0]
    cells_x, cells_y, depth = (species.shape[1], species.shape[2], species.shape[3])
    total_x = cells_x * lax.axis_size("gx")
    total_y = cells_y * lax.axis_size("gy")
    fields = jnp.concatenate([species, flow_fields], axis=0)
    padded = extended(fields, (("gx", 1), ("gy", 2)), 1)
    ahead_x = padded[:, 2:, 1:-1]
    behind_x = padded[:, :-2, 1:-1]
    ahead_y = padded[:, 1:-1, 2:]
    behind_y = padded[:, 1:-1, :-2]
    ahead_z = jnp.roll(fields, -1, 3)
    behind_z = jnp.roll(fields, 1, 3)
    stream_vel = flow_fields[1][None]
    span_vel = flow_fields[2][None]
    depth_vel = flow_fields[3][None]
    laplace_sum = ahead_x + behind_x + ahead_y + behind_y + ahead_z + behind_z - 6.0 * fields
    advection = 0.5 * (
        stream_vel * (ahead_x - behind_x)
        + span_vel * (ahead_y - behind_y)
        + depth_vel * (ahead_z - behind_z)
    )
    transported = fields + TIME_STEP * (diffusivity[:, None, None, None] * laplace_sum - advection)
    columns = cells_x * cells_y
    burning_mixture_status = jnp.concatenate(
        [transported[:nspec], transported[nspec + 4 : nspec + 5]], axis=0
    ).reshape(nspec + 1, columns, depth)
    class_flat = classes.reshape(columns)
    class_value = class_flat.astype(jnp.float32)
    burning_mixture_status = substep(
        burning_mixture_status, (TIME_STEP / class_value)[:, None], newton_matrix, params
    )
    stiff = class_flat > 1
    ranking = jnp.argsort(jnp.where(stiff, 0, 1).astype(jnp.int32), stable=True)
    stiff_count = jnp.sum(stiff.astype(jnp.int32))
    stiff_cap = columns // 2
    own_slots = ranking[:stiff_cap]
    live_slots = jnp.arange(stiff_cap) < stiff_count
    buffer = burning_mixture_status[:, own_slots]
    holding_category = jnp.where(live_slots, class_value[own_slots], 1.0)
    buffer = extras(buffer, holding_category, newton_matrix, params)
    burning_mixture_status = burning_mixture_status.at[:, own_slots].set(
        jnp.where(live_slots[None, :, None], buffer, burning_mixture_status[:, own_slots])
    )
    reacted = burning_mixture_status.reshape(nspec + 1, cells_x, cells_y, depth)
    source = (reacted[nspec] - transported[nspec + 4]) / TIME_STEP
    inputs = jnp.concatenate([transported[nspec + 1 : nspec + 4], source[None]], axis=0)
    spectra = forward_packed(inputs)
    spectra = stream_lines(lax.all_to_all(spectra, "gx", split_axis=4, concat_axis=2, tiled=True))
    spectra = span_lines(lax.all_to_all(spectra, "gy", split_axis=2, concat_axis=3, tiled=True))
    local_x = spectra.shape[2]
    local_z = spectra.shape[4]
    rows_x = lax.axis_index("gy") * local_x + jnp.arange(local_x, dtype=jnp.int32)
    rows_y = jnp.arange(total_y, dtype=jnp.int32)
    rows_z = lax.axis_index("gx") * local_z + jnp.arange(local_z, dtype=jnp.int32)
    projected = project(spectra, rows_x, total_x, rows_y, total_y, rows_z, depth)
    projected = backward(projected, 3)
    projected = stream_inverse(
        lax.all_to_all(projected, "gy", split_axis=3, concat_axis=2, tiled=True)
    )
    velocity = backward_packed(
        lax.all_to_all(projected, "gx", split_axis=2, concat_axis=4, tiled=True)
    )
    species_out = reacted[:nspec]
    flow_out = jnp.concatenate(
        [transported[nspec : nspec + 1], velocity, reacted[nspec : nspec + 1]], axis=0
    )
    return (species_out, flow_out)


F32 = jnp.float32
BF16 = jnp.bfloat16
SLOT = 16
GROUP = 24
PIECE = 80
WAVES = 3 * GROUP
ROWS = WAVES + SLOT
TILE = 8
LIVE = 6
FUSED_VMEM = 40 * 2**20
FINAL_VMEM = 16 * 2**20
MESH = pl.DeviceIdType.MESH


def split_constant(array):
    high = array.astype(ml_dtypes.bfloat16)
    low = (array - high.astype(np.float64)).astype(ml_dtypes.bfloat16)
    return high, low


def spectral_constants(grid_x, grid_y, cells_x, cells_y, depth):
    devices = grid_x * grid_y
    total_x, total_y = grid_x * cells_x, grid_y * cells_y
    z = np.arange(depth)
    m = np.arange(2 * devices)
    angle = 2 * np.pi * ((m[:, None] * z[None, :]) % depth) / depth
    alternate = np.where(z % 2 == 0, 1.0, -1.0)
    into = np.stack([np.cos(angle), -np.sin(angle)], 1)
    into[0, 1] = alternate
    back = np.stack([2 * np.cos(angle), -2 * np.sin(angle)], 1)
    back[0, 0] = 1.0
    back[0, 1] = alternate
    back = (back / (depth * total_x * total_y)).reshape(devices, 2, 2, depth)
    into = into.reshape(devices, 2, 2, depth)
    kz = (m * (2 * np.pi / depth)).reshape(devices, 2, 1)
    early = np.zeros((devices, TILE, 3, depth))
    late = np.zeros((devices, TILE, 2, depth))
    out = np.zeros((devices, TILE, 3, depth))
    early[:, 0:4, 0] = into.reshape(devices, 4, depth)
    out[:, 0:4, 0] = back.reshape(devices, 4, depth)
    for mode in (0, 1):
        early[:, 4:6, 1 + mode] = kz[:, mode, :, None] * into[:, mode]
        late[:, 4, mode] = -into[:, mode, 1] / TIME_STEP
        late[:, 5, mode] = into[:, mode, 0] / TIME_STEP
        out[:, 4:6, 1 + mode] = kz[:, mode, :, None] * back[:, mode]
    early, late, out = (a.reshape(devices * TILE, -1) for a in (early, late, out))

    gx, gy = np.arange(grid_x), np.arange(grid_y)
    xl, yl = np.arange(cells_x), np.arange(cells_y)
    wave = lambda a, b, n: np.exp(-2j * np.pi * ((a[:, None] * b[None, :]) % n) / n)
    left = np.kron(wave(gx, gx, grid_x), wave(gy, gy, grid_y))
    real = np.stack([np.stack([left.real, -left.imag], -1), np.stack([left.imag, left.real], -1)], -2)
    left = np.einsum("kgrs,pq->kprgqs", real, np.eye(TILE // 2)).reshape(TILE * devices, -1)
    twist = np.kron(wave(gx, xl, total_x), wave(gy, yl, total_y))
    twist = np.tile(twist, (1, 2))
    inner = np.kron(wave(xl, xl, cells_x), wave(yl, yl, cells_y))
    pair = np.eye(2)
    right = np.concatenate([np.kron(pair, inner.real), np.kron(pair, inner.imag)], 0)
    unright = np.concatenate([np.kron(pair, inner.real), -np.kron(pair, inner.imag)], 0)

    def waves(index, length):
        signed = np.where(index < (length + 1) // 2, index, index - length) * (2 * np.pi / length)
        return np.where(index == length // 2, 0.0, signed)

    kx = waves(gx[:, None] + grid_x * xl[None, :], total_x)
    ky = waves(gy[:, None] + grid_y * yl[None, :], total_y)
    shape = (grid_x, grid_y, cells_x, cells_y)
    kx = np.broadcast_to(kx[:, None, :, None], shape).reshape(devices, cells_x * cells_y)
    ky = np.broadcast_to(ky[None, :, None, :], shape).reshape(devices, cells_x * cells_y)
    kxy = np.concatenate([kx, ky], -1)
    square = np.concatenate([kx * kx + ky * ky] * 2, -1)
    matrices = []
    for matrix in (early, late, left, right, unright, left.T):
        matrices.extend(split_constant(matrix))
    matrices = np.ascontiguousarray(np.concatenate(matrices, 1))
    tables = np.ascontiguousarray(np.stack([twist.real, twist.imag, kxy, square]), dtype=np.float32)[:, :, None, :]
    return matrices, tables, *(np.ascontiguousarray(a) for a in split_constant(out))


def halves(value):
    high = value.astype(BF16)
    low = (value - high.astype(F32)).astype(BF16)
    return high, low


def mul(a, b):
    return jnp.dot(a, b, preferred_element_type=F32)


def mul_t(a, b):
    return lax.dot_general(a, b, (((1,), (1,)), ((), ())), preferred_element_type=F32)


def precise(a, b):
    return jnp.dot(a, b, precision=PRECISE, preferred_element_type=F32)


def turn(value):
    rows = value.shape[1]
    parity = lax.broadcasted_iota(jnp.int32, value.shape, 1) % 2
    return jnp.where(parity == 0, -pltpu.roll(value, rows - 1, 1), pltpu.roll(value, 1, 1))


def flame_kernel(
    grid_x, grid_y, species_hbm, flow_hbm, kinds_hbm, diffusivity_hbm, left_hbm, right_hbm, stoich_hbm, heat_hbm,
    prefactor_hbm, energy_hbm, newton_hbm, matrices_hbm, tables_hbm,
    species_out, flow_out, gathered_out,
    fields, moved, speed, halo_x, halo_y, edges, state, angles, trial, stacked, span,
    kinds, diffusivity, left_in, right_in, stoich_in, heat_in, prefactor_in, energy_in, newton_in,
    forms_t, newton_pad, weights_f, matrices, tables, inverse, packed, spectra, unpacked, gathered,
    load_sem, small_sem, big_sem, halo_send, halo_recv, out_send, out_recv, back_send, back_recv,
):
    devices = grid_x * grid_y
    gx, gy = lax.axis_index("gx"), lax.axis_index("gy")
    me = gx * grid_y + gy
    nspec = species_hbm.shape[0]
    nfield, columns, depth = fields.shape
    nflow = nfield - nspec
    cells_x, cells_y = kinds.shape
    nreac = heat_in.shape[1]

    def peer(offset):
        other = lax.rem(me + offset, devices)
        return other, {"gx": other // grid_y, "gy": lax.rem(other, grid_y)}

    barrier = pltpu.get_barrier_semaphore()
    loads = (
        pltpu.make_async_copy(species_hbm, fields.at[pl.ds(0, nspec)], load_sem.at[0]),
        pltpu.make_async_copy(flow_hbm, fields.at[pl.ds(nspec, nflow)], load_sem.at[1]),
    )
    for load in loads:
        load.start()
    smalls = []
    for source, target in (
        (diffusivity_hbm, diffusivity), (kinds_hbm, kinds), (left_hbm, left_in), (right_hbm, right_in),
        (stoich_hbm, stoich_in), (heat_hbm, heat_in), (prefactor_hbm, prefactor_in), (energy_hbm, energy_in),
        (newton_hbm, newton_in),
    ):
        smalls.append(pltpu.make_async_copy(source, target, small_sem.at[len(smalls)]))
        smalls[-1].start()
    bigs = (
        pltpu.make_async_copy(matrices_hbm, matrices, big_sem.at[0]),
        pltpu.make_async_copy(tables_hbm, tables, big_sem.at[1]),
    )

    @pl.loop(1, devices)
    def greet(offset):
        pl.semaphore_signal(barrier, inc=1, device_id=peer(offset)[1], device_id_type=MESH)

    state[...] = jnp.zeros_like(state)
    spectra[:, LIVE:TILE, :] = jnp.zeros((devices, TILE - LIVE, depth), F32)
    gathered[:, LIVE:TILE, :] = jnp.zeros((devices, TILE - LIVE, depth), F32)
    forms_t[...] = jnp.zeros_like(forms_t)
    newton_pad[...] = jnp.zeros_like(newton_pad)
    weights_f[...] = jnp.zeros_like(weights_f)
    for load in loads:
        load.wait()
    for big in bigs:
        big.start()
    for f in range(nfield):
        edges[0, f] = fields[f, pl.ds(0, cells_x, stride=cells_y), :]
        edges[1, f] = fields[f, pl.ds(cells_y - 1, cells_x, stride=cells_y), :]

    up_x = {"gx": lax.rem(gx + 1, grid_x), "gy": gy}
    down_x = {"gx": lax.rem(gx + grid_x - 1, grid_x), "gy": gy}
    up_y = {"gx": gx, "gy": lax.rem(gy + 1, grid_y)}
    down_y = {"gx": gx, "gy": lax.rem(gy + grid_y - 1, grid_y)}
    swaps = []
    for at, (source, target, device) in enumerate((
        (edges.at[1], halo_y.at[0], up_y),
        (edges.at[0], halo_y.at[1], down_y),
        (fields.at[:, pl.ds(columns - cells_y, cells_y)], halo_x.at[0], up_x),
        (fields.at[:, pl.ds(0, cells_y)], halo_x.at[1], down_x),
    )):
        swaps.append(pltpu.make_async_remote_copy(
            src_ref=source, dst_ref=target, send_sem=halo_send.at[at], recv_sem=halo_recv.at[at],
            device_id=device, device_id_type=MESH))

    def swap():
        pl.semaphore_wait(barrier, devices - 1)
        for copy in swaps:
            copy.start()

    reach = gx // 2 + gy // 2 + lax.rem(gy, 2)
    pl.when(reach >= 4)(swap)

    for small in smalls:
        small.wait()
    forms_t[0:nspec, 0:nreac] = left_in[...]
    forms_t[0:nspec, GROUP : GROUP + nreac] = right_in[...]
    forms_t[nspec : nspec + 1, 2 * GROUP : 2 * GROUP + nreac] = 0.5 * energy_in[...]
    base = forms_t[0:SLOT, :]
    high = base.astype(BF16).astype(F32)
    low = (base - high).astype(BF16).astype(F32)
    row = lax.broadcasted_iota(jnp.int32, (SLOT, depth), 0)
    lane = lax.broadcasted_iota(jnp.int32, (SLOT, depth), 1)
    forms_t[3 * SLOT : 4 * SLOT, :] = base + jnp.where(lane == row + WAVES, 1.0, 0.0)
    forms_t[0:SLOT, :] = high
    forms_t[SLOT : 2 * SLOT, :] = high
    forms_t[2 * SLOT : 3 * SLOT, :] = low
    turned_forms = jnp.transpose(forms_t[...])
    forms = turned_forms[:WAVES, : 3 * SLOT].astype(BF16)
    lift = turned_forms[:ROWS, 3 * SLOT : 4 * SLOT]
    forms_t[...] = jnp.zeros_like(forms_t)
    forms_t[0:nspec, 0:nreac] = stoich_in[...] * (0.5 * prefactor_in[...])
    forms_t[nspec : nspec + 1, 0:nreac] = heat_in[...] * (0.5 * prefactor_in[...])
    newton_pad[0 : nspec + 1, 0 : nspec + 1] = newton_in[...]
    newton = newton_pad[:, 0:SLOT]
    gain0 = precise(newton, forms_t[0:SLOT, :])
    gain1 = gain0 - precise(newton, gain0)
    gain2 = gain1 - precise(newton, gain1)
    gains = gain2 + pltpu.roll(gain1, GROUP, 1) + pltpu.roll(gain0, 2 * GROUP, 1)
    mixed = precise(lift, gains)
    high = mixed.astype(BF16).astype(F32)
    low = mixed - high
    for at in range(3):
        part = slice(at * GROUP, (at + 1) * GROUP)
        for place, value in enumerate((high, high, low)):
            begin = at * PIECE + place * GROUP
            weights_f[:, begin : begin + GROUP] = value[:, part]
    weights = weights_f[:, : 3 * PIECE].astype(BF16)
    last, middle = weights[:WAVES, 2 * PIECE :], weights[:WAVES, PIECE:]

    for axis in range(3):
        speed[axis] = fields[nspec + 1 + axis] * (0.5 * TIME_STEP)
    rows = lax.broadcasted_iota(jnp.int32, (cells_y, depth), 0)

    @pl.loop(0, nfield)
    def transport(f):
        coefficient = diffusivity[f] * TIME_STEP
        centre = 1.0 - 6.0 * coefficient
        for x in range(cells_x):
            at = pl.ds(x * cells_y, cells_y)
            here = fields[f, at]
            ahead_y = jnp.where(rows == cells_y - 1, 0.0, pltpu.roll(here, cells_y - 1, 0))
            behind_y = jnp.where(rows == 0, 0.0, pltpu.roll(here, 1, 0))
            ahead_z = pltpu.roll(here, depth - 1, 1)
            behind_z = pltpu.roll(here, 1, 1)
            total = ahead_y + behind_y + ahead_z + behind_z
            drift = speed[1, at] * (ahead_y - behind_y) + speed[2, at] * (ahead_z - behind_z)
            if 0 < x < cells_x - 1:
                ahead_x, behind_x = fields[f, pl.ds((x + 1) * cells_y, cells_y)], fields[f, pl.ds((x - 1) * cells_y, cells_y)]
                total = total + (ahead_x + behind_x)
                drift = drift + speed[0, at] * (ahead_x - behind_x)
            elif x == 0:
                ahead_x = fields[f, pl.ds(cells_y, cells_y)]
                total = total + ahead_x
                drift = drift + speed[0, at] * ahead_x
            else:
                behind_x = fields[f, pl.ds((x - 1) * cells_y, cells_y)]
                total = total + behind_x
                drift = drift - speed[0, at] * behind_x
            moved[f, at] = here * centre + (coefficient * total - drift)

    def source_of(f):
        return f if f < nspec else nfield - 1

    for f in range(nspec + 1):
        for x in range(1, cells_x - 1):
            state[pl.ds(x * cells_y * SLOT + f, cells_y, stride=SLOT), :] = moved[source_of(f), pl.ds(x * cells_y, cells_y)]

    def tile(column):
        return pl.ds(column * SLOT, SLOT)

    def rates(wave, step):
        curve = jnp.tanh(wave)
        rate = (1.0 + curve[2 * GROUP :]) * curve[:GROUP] * curve[GROUP : 2 * GROUP] * step
        high = rate.astype(BF16).astype(F32)
        low = rate - high
        pad = jnp.zeros((PIECE - 3 * GROUP, rate.shape[1]), F32)
        return jnp.concatenate([high, low, high, pad], axis=0).astype(BF16)

    def react(members):
        pairs = [members[i : i + 2] for i in range(0, len(members), 2)]
        wide = 2 * depth
        for at, pair in enumerate(pairs):
            value = jnp.concatenate([state[tile(c), :] for c in pair], axis=1)
            high, low = halves(value)
            angles[at] = mul(forms, jnp.concatenate([high, low, high], axis=0))
            for half, c in enumerate(pair):
                kind = jnp.full((TILE, depth), kinds[c // cells_y, c % cells_y], jnp.int32)
                span[at, :, half * depth : (half + 1) * depth] = kind.astype(F32)

        @pl.loop(0, 4)
        def section(number):
            limit = number.astype(F32)
            for at, pair in enumerate(pairs):
                spans = span[at]
                step = jnp.where(spans > limit, TIME_STEP / spans, 0.0)
                trial[at, WAVES:ROWS, :] = jnp.concatenate([step, step], axis=0)
                wave = angles[at]
                piece = rates(wave, jnp.concatenate([step] * 3, axis=0))
                stacked[at, 0:PIECE, :] = piece
                trial[at, 0:WAVES, :] = wave + mul(last, piece)
            for at, pair in enumerate(pairs):
                step = trial[at, WAVES : WAVES + TILE, :]
                stacked[at, PIECE : 2 * PIECE, :] = rates(trial[at, 0:WAVES, :], jnp.concatenate([step] * 3, axis=0))
                trial[at, 0:WAVES, :] = angles[at] + mul(middle, stacked[at, 0 : 2 * PIECE, :])
            for at, pair in enumerate(pairs):
                step = trial[at, WAVES : WAVES + TILE, :]
                stacked[at, 2 * PIECE : 3 * PIECE, :] = rates(trial[at, 0:WAVES, :], jnp.concatenate([step] * 3, axis=0))
                change = mul(weights, stacked[at])
                angles[at] = angles[at] + change[:WAVES]
                for half, c in enumerate(pair):
                    state[tile(c), :] = state[tile(c), :] + change[WAVES:, half * depth : (half + 1) * depth]

    pl.when(reach == 3)(swap)
    react([x * cells_y + y for x in range(1, cells_x - 1) for y in range(1, cells_y - 1)])
    pl.when(reach <= 2)(swap)

    for big in bigs:
        big.wait()
    lane = lax.broadcasted_iota(jnp.int32, (1, TILE, depth), 2)
    row = lax.broadcasted_iota(jnp.int32, (1, TILE, depth), 1)
    kz = (2 * me + row // 2).astype(F32) * (2.0 * np.pi / depth)
    square = tables[3] + kz * kz
    inverse[...] = 1.0 / jnp.where(square > 0, square, 1.0)

    for copy in swaps[2:]:
        copy.wait()
    for copy in swaps[:2]:
        copy.wait()
    first, final = pl.ds(0, cells_y), pl.ds(columns - cells_y, cells_y)
    low_y, high_y = pl.ds(0, cells_x, stride=cells_y), pl.ds(cells_y - 1, cells_x, stride=cells_y)
    for f in range(nfield):
        coefficient = diffusivity[f] * TIME_STEP
        moved[f, first] = moved[f, first] + halo_x[0, f] * (coefficient + speed[0, first])
        moved[f, final] = moved[f, final] + halo_x[1, f] * (coefficient - speed[0, final])
        moved[f, low_y, :] = moved[f, low_y, :] + halo_y[0, f] * (coefficient + speed[1, low_y, :])
        moved[f, high_y, :] = moved[f, high_y, :] + halo_y[1, f] * (coefficient - speed[1, high_y, :])
    for f in range(nspec + 1):
        source = source_of(f)
        for x in (0, cells_x - 1):
            state[pl.ds(x * cells_y * SLOT + f, cells_y, stride=SLOT), :] = moved[source, pl.ds(x * cells_y, cells_y)]
        for y in (0, cells_y - 1):
            state[pl.ds(y * SLOT + f, cells_x, stride=cells_y * SLOT), :] = moved[source, pl.ds(y, cells_x, stride=cells_y), :]

    sizes = [3 * depth, 3 * depth, 2 * depth, 2 * depth] + [2 * depth] * 2 + [depth] * 4 + [2 * depth] * 2
    starts = [sum(sizes[:i]) for i in range(len(sizes))]

    def matrix(at):
        return matrices[:, starts[at] : starts[at] + sizes[at]]

    def dot_left(at, value, product=mul):
        high, low = halves(value)
        a, b = matrix(at), matrix(at + 1)
        return product(a, high) + product(a, low) + product(b, high)

    def dot_right(value, at):
        high, low = halves(value)
        a, b = matrix(at), matrix(at + 1)
        return mul(high, a) + mul(low, a) + mul(high, b)

    none = jnp.zeros((columns, depth), F32)
    u, v, w = (moved[nspec + 1 + axis] for axis in range(3))
    lines = jnp.concatenate([jnp.concatenate([u, w, none], axis=1), jnp.concatenate([v, none, w], axis=1)], axis=0)
    packed[...] = dot_left(0, lines, mul_t).reshape(packed.shape)

    react([x * cells_y + y for x in (0, cells_x - 1) for y in range(1, cells_y - 1)]
          + [x * cells_y + y for y in (0, cells_y - 1) for x in range(cells_x)])

    for x in range(cells_x):
        hot = state[pl.ds(x * cells_y * SLOT + nspec, cells_y, stride=SLOT), :]
        flow_out[nflow - 1, pl.ds(x * cells_y, cells_y)] = hot
    warmth = flow_out[nflow - 1] - moved[nfield - 1]
    lines = jnp.concatenate([jnp.concatenate([warmth, none], axis=1), jnp.concatenate([none, warmth], axis=1)], axis=0)
    packed[...] = packed[...] + dot_left(2, lines, mul_t).reshape(packed.shape)

    live = pl.ds(0, LIVE)

    def exchange(source, target, send_sem, recv_sem, meanwhile):
        @pl.loop(1, devices)
        def start(offset):
            other, device = peer(offset)
            pltpu.make_async_remote_copy(
                src_ref=source.at[other, live], dst_ref=target.at[me, live],
                send_sem=send_sem.at[other], recv_sem=recv_sem.at[me],
                device_id=device, device_id_type=MESH).start()

        target[me, live] = source[me, live]
        meanwhile()

        @pl.loop(1, devices)
        def finish(offset):
            other, device = peer(offset)
            pltpu.make_async_remote_copy(
                src_ref=source.at[other, live], dst_ref=target.at[other, live],
                send_sem=send_sem.at[other], recv_sem=recv_sem.at[other],
                device_id=device, device_id_type=MESH).wait()

    def outputs():
        for f in range(nspec):
            for x in range(cells_x):
                species_out[f, pl.ds(x * cells_y, cells_y)] = state[pl.ds(x * cells_y * SLOT + f, cells_y, stride=SLOT), :]
        for f in range(nflow - 1):
            flow_out[f] = moved[nspec + f]

    exchange(packed, spectra, out_send, out_recv, outputs)

    shape = spectra.shape
    flat = (shape[0] * shape[1], shape[2])
    value = dot_left(4, spectra[...].reshape(flat)).reshape(shape)
    turned = turn(value)
    re, im = tables[0], tables[1]
    a = value * re + turned * im
    b = turned * re - value * im
    value = dot_right(jnp.concatenate([a.reshape(flat), b.reshape(flat)], axis=1), 6).reshape(shape)

    kxy = tables[2]
    upper = lane < columns
    total = kxy * value
    total = total + pltpu.roll(total, columns, 2)
    crossed = pltpu.roll(value, columns, 2)
    even = pltpu.roll(jnp.where(upper, value, crossed), 4, 1)
    odd = pltpu.roll(jnp.where(upper, crossed, value), 6, 1)
    potential = (total + jnp.where(row < 2, even, odd)) * inverse[...]
    deep = jnp.where(upper, pltpu.roll(potential, 4, 1), pltpu.roll(potential, 2, 1))
    value = jnp.where(row < 4, kxy * potential, jnp.where(row < LIVE, deep, 0.0))

    turned = turn(value)
    value = dot_right(jnp.concatenate([value.reshape(flat), turned.reshape(flat)], axis=1), 8).reshape(shape)
    value = value * re - turn(value) * im
    unpacked[...] = dot_left(10, value.reshape(flat)).reshape(shape)
    exchange(unpacked, gathered, back_send, back_recv, lambda: None)
    gathered_out[...] = gathered[...]


def final_kernel(back_h, back_l, species_in, flow_in, gathered, species_hbm, flow_hbm, flow, sems):
    nflow, columns, depth = flow.shape
    store = pltpu.make_async_copy(species_in, species_hbm, sems.at[0])
    store.start()
    value = jnp.transpose(gathered[...].reshape(back_h.shape[0], 2 * columns))
    high, low = halves(value)
    a, b = back_h[...], back_l[...]
    result = mul(high, a) + mul(low, a) + mul(high, b)
    flow[0] = flow_in[0]
    flow[1] = flow_in[1] - result[:columns, :depth]
    flow[2] = flow_in[2] - result[columns:, :depth]
    flow[3] = flow_in[3] - (result[:columns, depth : 2 * depth] + result[columns:, 2 * depth :])
    flow[4] = flow_in[4]
    ship = pltpu.make_async_copy(flow, flow_hbm, sems.at[1])
    ship.start()
    store.wait()
    ship.wait()


def flame(
    species, flow_fields, classes, diffusivity, left_form, right_form, stoich, heat_release,
    arrhenius_prefactor, arrhenius_energy, newton_matrix, matrices, tables, back_h, back_l,
):
    grid_x, grid_y = lax.axis_size("gx"), lax.axis_size("gy")
    nspec, cells_x, cells_y, depth = species.shape
    nflow = flow_fields.shape[0]
    nfield = nspec + nflow
    nreac = left_form.shape[0]
    columns = cells_x * cells_y
    devices = grid_x * grid_y
    hbm = pl.BlockSpec(memory_space=pltpu.HBM)
    vmem = pl.BlockSpec(memory_space=pltpu.VMEM)
    dma = pltpu.SemaphoreType.DMA
    box = (devices, TILE, depth)
    shaped = lambda shape: jax.ShapeDtypeStruct(shape, F32)
    line = lambda a: a.reshape(1, -1)
    inputs = (
        species.reshape(nspec, columns, depth), flow_fields.reshape(nflow, columns, depth), classes, diffusivity,
        left_form.T, right_form.T, stoich.T, line(heat_release), line(arrhenius_prefactor), line(arrhenius_energy),
        newton_matrix, matrices, tables,
    )
    most = (max((cells_x - 2) * (cells_y - 2), columns) + 1) // 2
    scratch = [
        pltpu.VMEM((nfield, columns, depth), F32),
        pltpu.VMEM((nfield, columns, depth), F32),
        pltpu.VMEM((3, columns, depth), F32),
        pltpu.VMEM((2, nfield, cells_y, depth), F32),
        pltpu.VMEM((2, nfield, cells_x, depth), F32),
        pltpu.VMEM((2, nfield, cells_x, depth), F32),
        pltpu.VMEM((columns * SLOT, depth), F32),
        pltpu.VMEM((most, WAVES, 2 * depth), F32),
        pltpu.VMEM((most, ROWS, 2 * depth), F32),
        pltpu.VMEM((most, 3 * PIECE, 2 * depth), BF16),
        pltpu.VMEM((most, TILE, 2 * depth), F32),
        pltpu.SMEM(classes.shape, jnp.int32),
        pltpu.SMEM(diffusivity.shape, F32),
    ]
    scratch += [pltpu.VMEM(a.shape, F32) for a in inputs[4:11]]
    scratch += [
        pltpu.VMEM((depth, depth), F32),
        pltpu.VMEM((SLOT, depth), F32),
        pltpu.VMEM((ROWS, 2 * depth), F32),
        pltpu.VMEM(matrices.shape, BF16),
        pltpu.VMEM(tables.shape, F32),
    ]
    scratch += [pltpu.VMEM(box, F32)] * 5
    scratch += [dma((2,)), dma((9,)), dma((2,)), dma((4,)), dma((4,))] + [dma((devices,))] * 4
    species_done, flow_done, gathered = pl.pallas_call(
        functools.partial(flame_kernel, grid_x, grid_y),
        out_shape=(shaped((nspec, columns, depth)), shaped((nflow, columns, depth)), shaped(box)),
        in_specs=[hbm] * len(inputs),
        out_specs=(vmem, vmem, vmem),
        scratch_shapes=scratch,
        compiler_params=pltpu.CompilerParams(collective_id=0, has_side_effects=True, vmem_limit_bytes=FUSED_VMEM),
        name="flame",
    )(*inputs)
    species_out, flow_out = pl.pallas_call(
        final_kernel,
        out_shape=(shaped((nspec, columns, depth)), shaped((nflow, columns, depth))),
        in_specs=[vmem] * 5,
        out_specs=(hbm, hbm),
        scratch_shapes=[pltpu.VMEM((nflow, columns, depth), F32), dma((2,))],
        compiler_params=pltpu.CompilerParams(vmem_limit_bytes=FINAL_VMEM),
        name="final",
    )(back_h, back_l, species_done, flow_done, gathered)
    return species_out.reshape(species.shape), flow_out.reshape(flow_fields.shape)


def solution(mesh):
    grid_x, grid_y = mesh.shape["gx"], mesh.shape["gy"]

    def step(species, flow_fields, classes, *rest):
        cells_x = species.shape[1] // grid_x
        cells_y = species.shape[2] // grid_y
        depth = species.shape[3]
        direct = (
            depth == 128 and cells_y == 8 and 2 * cells_x * cells_y == 128
            and depth == 4 * grid_x * grid_y
        )
        grids = (P(None, "gx", "gy", None), P(None, "gx", "gy", None), P("gx", "gy"))
        constants = ()
        if direct:
            constants = tuple(spectral_constants(grid_x, grid_y, cells_x, cells_y, depth))
        return jax.shard_map(
            flame if direct else shards,
            mesh=mesh,
            in_specs=grids + (P(),) * (len(rest) + len(constants)),
            out_specs=(P(None, "gx", "gy", None), P(None, "gx", "gy", None)),
            check_vma=False,
        )(species, flow_fields, classes, *rest, *constants)

    return step
```

```python
import functools

import jax
import jax.numpy as jnp
import ml_dtypes
import numpy as np
from jax import lax
from jax.experimental import pallas as pl
from jax.experimental.pallas import tpu as pltpu
from jax.sharding import PartitionSpec as P

TIME_STEP = 0.25
PRECISE = lax.Precision.HIGHEST


def extended(value, sides, width):
    for axis, dim in sides:
        size, length = (lax.axis_size(axis), value.shape[dim])
        up = [(i, (i + 1) % size) for i in range(size)]
        down = [(j, i) for i, j in up]
        last = lax.slice_in_dim(value, length - width, length, axis=dim)
        first = lax.slice_in_dim(value, 0, width, axis=dim)
        before = lax.ppermute(last, axis, up)
        after = lax.ppermute(first, axis, down)
        value = jnp.concatenate([before, value, after], axis=dim)
    return value


def reaction_rates(burning_mixture_status, params):
    left_form, right_form, stoich, heat_release, arrhenius_prefactor, arrhenius_energy = params
    fractions = burning_mixture_status[:-1]
    thermal_kelvin_field = burning_mixture_status[-1]
    left_sum = jnp.tanh(jnp.einsum("rs,scn->rcn", left_form, fractions, precision=PRECISE))
    right_sum = jnp.tanh(jnp.einsum("rs,scn->rcn", right_form, fractions, precision=PRECISE))
    flow_speed_norm = arrhenius_prefactor[:, None, None] * jax.nn.sigmoid(
        arrhenius_energy[:, None, None] * thermal_kelvin_field[None]
    )
    progress = flow_speed_norm * left_sum * right_sum
    species_rate = jnp.einsum("rs,rcn->scn", stoich, progress, precision=PRECISE)
    heat_rate = jnp.einsum("r,rcn->cn", heat_release, progress, precision=PRECISE)
    return jnp.concatenate([species_rate, heat_rate[None]], axis=0)


def substep(start, step_size, newton_matrix, params):
    current = start
    for repeat in range(3):
        residue = current - start - step_size[None] * reaction_rates(current, params)
        current = current - jnp.einsum("ij,jcn->icn", newton_matrix, residue, precision=PRECISE)
    return current


def extras(buffer, class_value, newton_matrix, params):
    step_size = (TIME_STEP / class_value)[:, None]
    for section in (1, 2, 3):
        active = (class_value > section)[None, :, None]
        buffer = jnp.where(active, substep(buffer, step_size, newton_matrix, params), buffer)
    return buffer


def tables(length):
    index = jnp.arange(length, dtype=jnp.int32)
    phase = index[:, None] * index[None, :] % length
    angle = phase.astype(jnp.float32) * (2.0 * jnp.pi / length)
    return (jnp.cos(angle), jnp.sin(angle))


def half_angles(length):
    index = jnp.arange(length, dtype=jnp.int32)
    modes = jnp.arange(length // 2, dtype=jnp.int32)
    phase = index[:, None] * modes[None, :] % length
    angle = phase.astype(jnp.float32) * (2.0 * jnp.pi / length)
    alternate = jnp.where(index % 2 == 0, 1.0, -1.0).astype(jnp.float32)
    return (angle, alternate, modes)


def transform_dim(array, dimension, lookup):
    moved_last = jnp.moveaxis(array, dimension, -1)
    result = jnp.einsum("...j,jk->...k", moved_last, lookup, precision=PRECISE)
    return jnp.moveaxis(result, -1, dimension)


def forward(spectra, dimension):
    length = spectra.shape[dimension]
    cosine, sine_table = tables(length)
    real_part = spectra[:, 0]
    imag_part = spectra[:, 1]
    inner = dimension - 1
    new_real = transform_dim(real_part, inner, cosine) + transform_dim(imag_part, inner, sine_table)
    new_imag = transform_dim(imag_part, inner, cosine) - transform_dim(real_part, inner, sine_table)
    return jnp.stack([new_real, new_imag], axis=1)


def backward(spectra, dimension):
    length = spectra.shape[dimension]
    cosine, sine_table = tables(length)
    real_part = spectra[:, 0]
    imag_part = spectra[:, 1]
    inner = dimension - 1
    new_real = (
        transform_dim(real_part, inner, cosine) - transform_dim(imag_part, inner, sine_table)
    ) / length
    new_imag = (
        transform_dim(imag_part, inner, cosine) + transform_dim(real_part, inner, sine_table)
    ) / length
    return jnp.stack([new_real, new_imag], axis=1)


def forward_packed(values):
    length = values.shape[3]
    angle, alternate, modes = half_angles(length)
    cosine = jnp.cos(angle)
    packed_sine = jnp.where(modes[None, :] == 0, -alternate[:, None], jnp.sin(angle))
    return jnp.stack(
        [transform_dim(values, 3, cosine), -transform_dim(values, 3, packed_sine)], axis=1
    )


def backward_packed(spectra):
    length = 2 * spectra.shape[4]
    angle, alternate, modes = half_angles(length)
    weight = jnp.where(modes == 0, 1.0, 2.0).astype(jnp.float32)
    cos_back = weight[:, None] * jnp.cos(angle.T)
    sin_back = jnp.where(modes[:, None] == 0, -alternate[None, :], 2.0 * jnp.sin(angle.T))
    return (
        transform_dim(spectra[:, 0], 3, cos_back) - transform_dim(spectra[:, 1], 3, sin_back)
    ) / length


def wave_numbers(index, length):
    signed = jnp.where(index < (length + 1) // 2, index, index - length)
    waves = signed.astype(jnp.float32) * (2.0 * jnp.pi / length)
    return jnp.where(index == length // 2, 0.0, waves)


def project(spectra, rows_x, total_x, rows_y, total_y, rows_z, total_z):
    wave_x = wave_numbers(rows_x, total_x)[:, None, None]
    wave_y = wave_numbers(rows_y, total_y)[None, :, None]
    wave_z = wave_numbers(rows_z, total_z)[None, None, :]
    wavenumber_squared = wave_x * wave_x + wave_y * wave_y + wave_z * wave_z
    denom = jnp.where(wavenumber_squared > 0, wavenumber_squared, 1.0)
    vel_real = spectra[:3, 0]
    vel_imag = spectra[:3, 1]
    source_real = spectra[3, 0]
    source_imag = spectra[3, 1]
    inner_product_real = wave_x * vel_real[0] + wave_y * vel_real[1] + wave_z * vel_real[2]
    imaginary_inner_sum = wave_x * vel_imag[0] + wave_y * vel_imag[1] + wave_z * vel_imag[2]
    waves = (wave_x, wave_y, wave_z)
    outputs = []
    for axis in range(3):
        out_real = (
            vel_real[axis]
            - waves[axis] * inner_product_real / denom
            + waves[axis] * source_imag / denom
        )
        out_imag = (
            vel_imag[axis]
            - waves[axis] * imaginary_inner_sum / denom
            - waves[axis] * source_real / denom
        )
        outputs.append(jnp.stack([out_real, out_imag], axis=0))
    return jnp.stack(outputs, axis=0)


def stream_lines(spectra):
    return forward(spectra, 2)


def span_lines(spectra):
    return forward(spectra, 3)


def stream_inverse(spectra):
    return backward(spectra, 2)


def shards(
    species,
    flow_fields,
    classes,
    diffusivity,
    left_form,
    right_form,
    stoich,
    heat_release,
    arrhenius_prefactor,
    arrhenius_energy,
    newton_matrix,
):
    params = (left_form, right_form, stoich, heat_release, arrhenius_prefactor, arrhenius_energy)
    nspec = species.shape[0]
    cells_x, cells_y, depth = (species.shape[1], species.shape[2], species.shape[3])
    total_x = cells_x * lax.axis_size("gx")
    total_y = cells_y * lax.axis_size("gy")
    fields = jnp.concatenate([species, flow_fields], axis=0)
    padded = extended(fields, (("gx", 1), ("gy", 2)), 1)
    ahead_x = padded[:, 2:, 1:-1]
    behind_x = padded[:, :-2, 1:-1]
    ahead_y = padded[:, 1:-1, 2:]
    behind_y = padded[:, 1:-1, :-2]
    ahead_z = jnp.roll(fields, -1, 3)
    behind_z = jnp.roll(fields, 1, 3)
    stream_vel = flow_fields[1][None]
    span_vel = flow_fields[2][None]
    depth_vel = flow_fields[3][None]
    laplace_sum = ahead_x + behind_x + ahead_y + behind_y + ahead_z + behind_z - 6.0 * fields
    advection = 0.5 * (
        stream_vel * (ahead_x - behind_x)
        + span_vel * (ahead_y - behind_y)
        + depth_vel * (ahead_z - behind_z)
    )
    transported = fields + TIME_STEP * (diffusivity[:, None, None, None] * laplace_sum - advection)
    columns = cells_x * cells_y
    burning_mixture_status = jnp.concatenate(
        [transported[:nspec], transported[nspec + 4 : nspec + 5]], axis=0
    ).reshape(nspec + 1, columns, depth)
    class_flat = classes.reshape(columns)
    class_value = class_flat.astype(jnp.float32)
    burning_mixture_status = substep(
        burning_mixture_status, (TIME_STEP / class_value)[:, None], newton_matrix, params
    )
    stiff = class_flat > 1
    ranking = jnp.argsort(jnp.where(stiff, 0, 1).astype(jnp.int32), stable=True)
    stiff_count = jnp.sum(stiff.astype(jnp.int32))
    stiff_cap = columns // 2
    own_slots = ranking[:stiff_cap]
    live_slots = jnp.arange(stiff_cap) < stiff_count
    buffer = burning_mixture_status[:, own_slots]
    holding_category = jnp.where(live_slots, class_value[own_slots], 1.0)
    buffer = extras(buffer, holding_category, newton_matrix, params)
    burning_mixture_status = burning_mixture_status.at[:, own_slots].set(
        jnp.where(live_slots[None, :, None], buffer, burning_mixture_status[:, own_slots])
    )
    reacted = burning_mixture_status.reshape(nspec + 1, cells_x, cells_y, depth)
    source = (reacted[nspec] - transported[nspec + 4]) / TIME_STEP
    inputs = jnp.concatenate([transported[nspec + 1 : nspec + 4], source[None]], axis=0)
    spectra = forward_packed(inputs)
    spectra = stream_lines(lax.all_to_all(spectra, "gx", split_axis=4, concat_axis=2, tiled=True))
    spectra = span_lines(lax.all_to_all(spectra, "gy", split_axis=2, concat_axis=3, tiled=True))
    local_x = spectra.shape[2]
    local_z = spectra.shape[4]
    rows_x = lax.axis_index("gy") * local_x + jnp.arange(local_x, dtype=jnp.int32)
    rows_y = jnp.arange(total_y, dtype=jnp.int32)
    rows_z = lax.axis_index("gx") * local_z + jnp.arange(local_z, dtype=jnp.int32)
    projected = project(spectra, rows_x, total_x, rows_y, total_y, rows_z, depth)
    projected = backward(projected, 3)
    projected = stream_inverse(
        lax.all_to_all(projected, "gy", split_axis=3, concat_axis=2, tiled=True)
    )
    velocity = backward_packed(
        lax.all_to_all(projected, "gx", split_axis=2, concat_axis=4, tiled=True)
    )
    species_out = reacted[:nspec]
    flow_out = jnp.concatenate(
        [transported[nspec : nspec + 1], velocity, reacted[nspec : nspec + 1]], axis=0
    )
    return (species_out, flow_out)


F32 = jnp.float32
BF16 = jnp.bfloat16
SLOT = 16
GROUP = 24
PIECE = 80
WAVES = 3 * GROUP
ROWS = WAVES + SLOT
TILE = 8
LIVE = 6
FUSED_VMEM = 40 * 2**20
FINAL_VMEM = 16 * 2**20
MESH = pl.DeviceIdType.MESH


def split_constant(array):
    high = array.astype(ml_dtypes.bfloat16)
    low = (array - high.astype(np.float64)).astype(ml_dtypes.bfloat16)
    return high, low


def spectral_constants(grid_x, grid_y, cells_x, cells_y, depth):
    devices = grid_x * grid_y
    total_x, total_y = grid_x * cells_x, grid_y * cells_y
    z = np.arange(depth)
    m = np.arange(2 * devices)
    angle = 2 * np.pi * ((m[:, None] * z[None, :]) % depth) / depth
    alternate = np.where(z % 2 == 0, 1.0, -1.0)
    into = np.stack([np.cos(angle), -np.sin(angle)], 1)
    into[0, 1] = alternate
    back = np.stack([2 * np.cos(angle), -2 * np.sin(angle)], 1)
    back[0, 0] = 1.0
    back[0, 1] = alternate
    back = (back / (depth * total_x * total_y)).reshape(devices, 2, 2, depth)
    into = into.reshape(devices, 2, 2, depth)
    kz = (m * (2 * np.pi / depth)).reshape(devices, 2, 1)
    early = np.zeros((devices, TILE, 3, depth))
    late = np.zeros((devices, TILE, 2, depth))
    out = np.zeros((devices, TILE, 3, depth))
    early[:, 0:4, 0] = into.reshape(devices, 4, depth)
    out[:, 0:4, 0] = back.reshape(devices, 4, depth)
    for mode in (0, 1):
        early[:, 4:6, 1 + mode] = kz[:, mode, :, None] * into[:, mode]
        late[:, 4, mode] = -into[:, mode, 1] / TIME_STEP
        late[:, 5, mode] = into[:, mode, 0] / TIME_STEP
        out[:, 4:6, 1 + mode] = kz[:, mode, :, None] * back[:, mode]
    early, late, out = (a.reshape(devices * TILE, -1) for a in (early, late, out))

    gx, gy = np.arange(grid_x), np.arange(grid_y)
    xl, yl = np.arange(cells_x), np.arange(cells_y)
    wave = lambda a, b, n: np.exp(-2j * np.pi * ((a[:, None] * b[None, :]) % n) / n)
    left = np.kron(wave(gx, gx, grid_x), wave(gy, gy, grid_y))
    real = np.stack([np.stack([left.real, -left.imag], -1), np.stack([left.imag, left.real], -1)], -2)
    left = np.einsum("kgrs,pq->kprgqs", real, np.eye(TILE // 2)).reshape(TILE * devices, -1)
    twist = np.kron(wave(gx, xl, total_x), wave(gy, yl, total_y))
    twist = np.tile(twist, (1, 2))
    inner = np.kron(wave(xl, xl, cells_x), wave(yl, yl, cells_y))
    pair = np.eye(2)
    right = np.concatenate([np.kron(pair, inner.real), np.kron(pair, inner.imag)], 0)
    unright = np.concatenate([np.kron(pair, inner.real), -np.kron(pair, inner.imag)], 0)

    def waves(index, length):
        signed = np.where(index < (length + 1) // 2, index, index - length) * (2 * np.pi / length)
        return np.where(index == length // 2, 0.0, signed)

    kx = waves(gx[:, None] + grid_x * xl[None, :], total_x)
    ky = waves(gy[:, None] + grid_y * yl[None, :], total_y)
    shape = (grid_x, grid_y, cells_x, cells_y)
    kx = np.broadcast_to(kx[:, None, :, None], shape).reshape(devices, cells_x * cells_y)
    ky = np.broadcast_to(ky[None, :, None, :], shape).reshape(devices, cells_x * cells_y)
    kxy = np.concatenate([kx, ky], -1)
    square = np.concatenate([kx * kx + ky * ky] * 2, -1)
    matrices = []
    for matrix in (early, late, left, right, unright, left.T):
        matrices.extend(split_constant(matrix))
    matrices = np.ascontiguousarray(np.concatenate(matrices, 1))
    tables = np.ascontiguousarray(np.stack([twist.real, twist.imag, kxy, square]), dtype=np.float32)[:, :, None, :]
    return matrices, tables, *(np.ascontiguousarray(a) for a in split_constant(out))


def halves(value):
    high = value.astype(BF16)
    low = (value - high.astype(F32)).astype(BF16)
    return high, low


def mul(a, b):
    return jnp.dot(a, b, preferred_element_type=F32)


def mul_t(a, b):
    return lax.dot_general(a, b, (((1,), (1,)), ((), ())), preferred_element_type=F32)


def precise(a, b):
    return jnp.dot(a, b, precision=PRECISE, preferred_element_type=F32)


def turn(value):
    rows = value.shape[1]
    parity = lax.broadcasted_iota(jnp.int32, value.shape, 1) % 2
    return jnp.where(parity == 0, -pltpu.roll(value, rows - 1, 1), pltpu.roll(value, 1, 1))


def flame_kernel(
    grid_x, grid_y, species_hbm, flow_hbm, kinds_hbm, diffusivity_hbm, left_hbm, right_hbm, stoich_hbm, heat_hbm,
    prefactor_hbm, energy_hbm, newton_hbm, matrices_hbm, tables_hbm,
    species_out, flow_out, gathered_out,
    fields, moved, speed, halo_x, halo_y, edges, state, angles, trial, stacked, span,
    kinds, diffusivity, left_in, right_in, stoich_in, heat_in, prefactor_in, energy_in, newton_in,
    forms_t, newton_pad, weights_f, matrices, tables, inverse, packed, spectra, unpacked, gathered,
    load_sem, small_sem, big_sem, halo_send, halo_recv, out_send, out_recv, back_send, back_recv,
):
    devices = grid_x * grid_y
    gx, gy = lax.axis_index("gx"), lax.axis_index("gy")
    me = gx * grid_y + gy
    nspec = species_hbm.shape[0]
    nfield, columns, depth = fields.shape
    nflow = nfield - nspec
    cells_x, cells_y = kinds.shape
    nreac = heat_in.shape[1]

    def peer(offset):
        other = lax.rem(me + offset, devices)
        return other, {"gx": other // grid_y, "gy": lax.rem(other, grid_y)}

    barrier = pltpu.get_barrier_semaphore()
    loads = (
        pltpu.make_async_copy(species_hbm, fields.at[pl.ds(0, nspec)], load_sem.at[0]),
        pltpu.make_async_copy(flow_hbm, fields.at[pl.ds(nspec, nflow)], load_sem.at[1]),
    )
    for load in loads:
        load.start()
    smalls = []
    for source, target in (
        (diffusivity_hbm, diffusivity), (kinds_hbm, kinds), (left_hbm, left_in), (right_hbm, right_in),
        (stoich_hbm, stoich_in), (heat_hbm, heat_in), (prefactor_hbm, prefactor_in), (energy_hbm, energy_in),
        (newton_hbm, newton_in),
    ):
        smalls.append(pltpu.make_async_copy(source, target, small_sem.at[len(smalls)]))
        smalls[-1].start()
    bigs = (
        pltpu.make_async_copy(matrices_hbm, matrices, big_sem.at[0]),
        pltpu.make_async_copy(tables_hbm, tables, big_sem.at[1]),
    )

    @pl.loop(1, devices)
    def greet(offset):
        pl.semaphore_signal(barrier, inc=1, device_id=peer(offset)[1], device_id_type=MESH)

    state[...] = jnp.zeros_like(state)
    spectra[:, LIVE:TILE, :] = jnp.zeros((devices, TILE - LIVE, depth), F32)
    gathered[:, LIVE:TILE, :] = jnp.zeros((devices, TILE - LIVE, depth), F32)
    forms_t[...] = jnp.zeros_like(forms_t)
    newton_pad[...] = jnp.zeros_like(newton_pad)
    weights_f[...] = jnp.zeros_like(weights_f)
    for load in loads:
        load.wait()
    for big in bigs:
        big.start()
    for f in range(nfield):
        edges[0, f] = fields[f, pl.ds(0, cells_x, stride=cells_y), :]
        edges[1, f] = fields[f, pl.ds(cells_y - 1, cells_x, stride=cells_y), :]

    up_x = {"gx": lax.rem(gx + 1, grid_x), "gy": gy}
    down_x = {"gx": lax.rem(gx + grid_x - 1, grid_x), "gy": gy}
    up_y = {"gx": gx, "gy": lax.rem(gy + 1, grid_y)}
    down_y = {"gx": gx, "gy": lax.rem(gy + grid_y - 1, grid_y)}
    swaps = []
    for at, (source, target, device) in enumerate((
        (edges.at[1], halo_y.at[0], up_y),
        (edges.at[0], halo_y.at[1], down_y),
        (fields.at[:, pl.ds(columns - cells_y, cells_y)], halo_x.at[0], up_x),
        (fields.at[:, pl.ds(0, cells_y)], halo_x.at[1], down_x),
    )):
        swaps.append(pltpu.make_async_remote_copy(
            src_ref=source, dst_ref=target, send_sem=halo_send.at[at], recv_sem=halo_recv.at[at],
            device_id=device, device_id_type=MESH))

    def swap():
        pl.semaphore_wait(barrier, devices - 1)
        for copy in swaps:
            copy.start()

    reach = gx // 2 + gy // 2 + lax.rem(gy, 2)
    pl.when(reach >= 4)(swap)

    for small in smalls:
        small.wait()
    forms_t[0:nspec, 0:nreac] = left_in[...]
    forms_t[0:nspec, GROUP : GROUP + nreac] = right_in[...]
    forms_t[nspec : nspec + 1, 2 * GROUP : 2 * GROUP + nreac] = 0.5 * energy_in[...]
    base = forms_t[0:SLOT, :]
    high = base.astype(BF16).astype(F32)
    low = (base - high).astype(BF16).astype(F32)
    row = lax.broadcasted_iota(jnp.int32, (SLOT, depth), 0)
    lane = lax.broadcasted_iota(jnp.int32, (SLOT, depth), 1)
    forms_t[3 * SLOT : 4 * SLOT, :] = base + jnp.where(lane == row + WAVES, 1.0, 0.0)
    forms_t[0:SLOT, :] = high
    forms_t[SLOT : 2 * SLOT, :] = high
    forms_t[2 * SLOT : 3 * SLOT, :] = low
    turned_forms = jnp.transpose(forms_t[...])
    forms = turned_forms[:WAVES, : 3 * SLOT].astype(BF16)
    lift = turned_forms[:ROWS, 3 * SLOT : 4 * SLOT]
    forms_t[...] = jnp.zeros_like(forms_t)
    forms_t[0:nspec, 0:nreac] = stoich_in[...] * (0.5 * prefactor_in[...])
    forms_t[nspec : nspec + 1, 0:nreac] = heat_in[...] * (0.5 * prefactor_in[...])
    newton_pad[0 : nspec + 1, 0 : nspec + 1] = newton_in[...]
    newton = newton_pad[:, 0:SLOT]
    gain0 = precise(newton, forms_t[0:SLOT, :])
    gain1 = gain0 - precise(newton, gain0)
    gain2 = gain1 - precise(newton, gain1)
    gains = gain2 + pltpu.roll(gain1, GROUP, 1) + pltpu.roll(gain0, 2 * GROUP, 1)
    mixed = precise(lift, gains)
    high = mixed.astype(BF16).astype(F32)
    low = mixed - high
    for at in range(3):
        part = slice(at * GROUP, (at + 1) * GROUP)
        for place, value in enumerate((high, high, low)):
            begin = at * PIECE + place * GROUP
            weights_f[:, begin : begin + GROUP] = value[:, part]
    weights = weights_f[:, : 3 * PIECE].astype(BF16)
    last, middle = weights[:WAVES, 2 * PIECE :], weights[:WAVES, PIECE:]

    for axis in range(3):
        speed[axis] = fields[nspec + 1 + axis] * (0.5 * TIME_STEP)
    rows = lax.broadcasted_iota(jnp.int32, (cells_y, depth), 0)

    @pl.loop(0, nfield)
    def transport(f):
        coefficient = diffusivity[f] * TIME_STEP
        centre = 1.0 - 6.0 * coefficient
        for x in range(cells_x):
            at = pl.ds(x * cells_y, cells_y)
            here = fields[f, at]
            ahead_y = jnp.where(rows == cells_y - 1, 0.0, pltpu.roll(here, cells_y - 1, 0))
            behind_y = jnp.where(rows == 0, 0.0, pltpu.roll(here, 1, 0))
            ahead_z = pltpu.roll(here, depth - 1, 1)
            behind_z = pltpu.roll(here, 1, 1)
            total = ahead_y + behind_y + ahead_z + behind_z
            drift = speed[1, at] * (ahead_y - behind_y) + speed[2, at] * (ahead_z - behind_z)
            if 0 < x < cells_x - 1:
                ahead_x, behind_x = fields[f, pl.ds((x + 1) * cells_y, cells_y)], fields[f, pl.ds((x - 1) * cells_y, cells_y)]
                total = total + (ahead_x + behind_x)
                drift = drift + speed[0, at] * (ahead_x - behind_x)
            elif x == 0:
                ahead_x = fields[f, pl.ds(cells_y, cells_y)]
                total = total + ahead_x
                drift = drift + speed[0, at] * ahead_x
            else:
                behind_x = fields[f, pl.ds((x - 1) * cells_y, cells_y)]
                total = total + behind_x
                drift = drift - speed[0, at] * behind_x
            moved[f, at] = here * centre + (coefficient * total - drift)

    def source_of(f):
        return f if f < nspec else nfield - 1

    for f in range(nspec + 1):
        for x in range(1, cells_x - 1):
            state[pl.ds(x * cells_y * SLOT + f, cells_y, stride=SLOT), :] = moved[source_of(f), pl.ds(x * cells_y, cells_y)]

    def tile(column):
        return pl.ds(column * SLOT, SLOT)

    def rates(wave, step):
        curve = jnp.tanh(wave)
        rate = (1.0 + curve[2 * GROUP :]) * curve[:GROUP] * curve[GROUP : 2 * GROUP] * step
        high = rate.astype(BF16).astype(F32)
        low = rate - high
        pad = jnp.zeros((PIECE - 3 * GROUP, rate.shape[1]), F32)
        return jnp.concatenate([high, low, high, pad], axis=0).astype(BF16)

    def react(members):
        pairs = [members[i : i + 2] for i in range(0, len(members), 2)]
        wide = 2 * depth
        for at, pair in enumerate(pairs):
            value = jnp.concatenate([state[tile(c), :] for c in pair], axis=1)
            high, low = halves(value)
            angles[at] = mul(forms, jnp.concatenate([high, low, high], axis=0))
            for half, c in enumerate(pair):
                kind = jnp.full((TILE, depth), kinds[c // cells_y, c % cells_y], jnp.int32)
                span[at, :, half * depth : (half + 1) * depth] = kind.astype(F32)

        @pl.loop(0, 4)
        def section(number):
            limit = number.astype(F32)
            for at, pair in enumerate(pairs):
                spans = span[at]
                step = jnp.where(spans > limit, TIME_STEP / spans, 0.0)
                trial[at, WAVES:ROWS, :] = jnp.concatenate([step, step], axis=0)
                wave = angles[at]
                piece = rates(wave, jnp.concatenate([step] * 3, axis=0))
                stacked[at, 0:PIECE, :] = piece
                trial[at, 0:WAVES, :] = wave + mul(last, piece)
            for at, pair in enumerate(pairs):
                step = trial[at, WAVES : WAVES + TILE, :]
                stacked[at, PIECE : 2 * PIECE, :] = rates(trial[at, 0:WAVES, :], jnp.concatenate([step] * 3, axis=0))
                trial[at, 0:WAVES, :] = angles[at] + mul(middle, stacked[at, 0 : 2 * PIECE, :])
            for at, pair in enumerate(pairs):
                step = trial[at, WAVES : WAVES + TILE, :]
                stacked[at, 2 * PIECE : 3 * PIECE, :] = rates(trial[at, 0:WAVES, :], jnp.concatenate([step] * 3, axis=0))
                change = mul(weights, stacked[at])
                angles[at] = angles[at] + change[:WAVES]
                for half, c in enumerate(pair):
                    state[tile(c), :] = state[tile(c), :] + change[WAVES:, half * depth : (half + 1) * depth]

    pl.when(reach == 3)(swap)
    react([x * cells_y + y for x in range(1, cells_x - 1) for y in range(1, cells_y - 1)])
    pl.when(reach <= 2)(swap)

    for big in bigs:
        big.wait()
    lane = lax.broadcasted_iota(jnp.int32, (1, TILE, depth), 2)
    row = lax.broadcasted_iota(jnp.int32, (1, TILE, depth), 1)
    kz = (2 * me + row // 2).astype(F32) * (2.0 * np.pi / depth)
    square = tables[3] + kz * kz
    inverse[...] = 1.0 / jnp.where(square > 0, square, 1.0)

    for copy in swaps[2:]:
        copy.wait()
    for copy in swaps[:2]:
        copy.wait()
    first, final = pl.ds(0, cells_y), pl.ds(columns - cells_y, cells_y)
    low_y, high_y = pl.ds(0, cells_x, stride=cells_y), pl.ds(cells_y - 1, cells_x, stride=cells_y)
    for f in range(nfield):
        coefficient = diffusivity[f] * TIME_STEP
        moved[f, first] = moved[f, first] + halo_x[0, f] * (coefficient + speed[0, first])
        moved[f, final] = moved[f, final] + halo_x[1, f] * (coefficient - speed[0, final])
        moved[f, low_y, :] = moved[f, low_y, :] + halo_y[0, f] * (coefficient + speed[1, low_y, :])
        moved[f, high_y, :] = moved[f, high_y, :] + halo_y[1, f] * (coefficient - speed[1, high_y, :])
    for f in range(nspec + 1):
        source = source_of(f)
        for x in (0, cells_x - 1):
            state[pl.ds(x * cells_y * SLOT + f, cells_y, stride=SLOT), :] = moved[source, pl.ds(x * cells_y, cells_y)]
        for y in (0, cells_y - 1):
            state[pl.ds(y * SLOT + f, cells_x, stride=cells_y * SLOT), :] = moved[source, pl.ds(y, cells_x, stride=cells_y), :]

    sizes = [3 * depth, 3 * depth, 2 * depth, 2 * depth] + [2 * depth] * 2 + [depth] * 4 + [2 * depth] * 2
    starts = [sum(sizes[:i]) for i in range(len(sizes))]

    def matrix(at):
        return matrices[:, starts[at] : starts[at] + sizes[at]]

    def dot_left(at, value, product=mul):
        high, low = halves(value)
        a, b = matrix(at), matrix(at + 1)
        return product(a, high) + product(a, low) + product(b, high)

    def dot_right(value, at):
        high, low = halves(value)
        a, b = matrix(at), matrix(at + 1)
        return mul(high, a) + mul(low, a) + mul(high, b)

    none = jnp.zeros((columns, depth), F32)
    u, v, w = (moved[nspec + 1 + axis] for axis in range(3))
    lines = jnp.concatenate([jnp.concatenate([u, w, none], axis=1), jnp.concatenate([v, none, w], axis=1)], axis=0)
    packed[...] = dot_left(0, lines, mul_t).reshape(packed.shape)

    react([x * cells_y + y for x in (0, cells_x - 1) for y in range(1, cells_y - 1)]
          + [x * cells_y + y for y in (0, cells_y - 1) for x in range(cells_x)])

    for x in range(cells_x):
        hot = state[pl.ds(x * cells_y * SLOT + nspec, cells_y, stride=SLOT), :]
        flow_out[nflow - 1, pl.ds(x * cells_y, cells_y)] = hot
    warmth = flow_out[nflow - 1] - moved[nfield - 1]
    lines = jnp.concatenate([jnp.concatenate([warmth, none], axis=1), jnp.concatenate([none, warmth], axis=1)], axis=0)
    packed[...] = packed[...] + dot_left(2, lines, mul_t).reshape(packed.shape)

    live = pl.ds(0, LIVE)

    def exchange(source, target, send_sem, recv_sem, meanwhile):
        @pl.loop(1, devices)
        def start(offset):
            other, device = peer(offset)
            pltpu.make_async_remote_copy(
                src_ref=source.at[other, live], dst_ref=target.at[me, live],
                send_sem=send_sem.at[other], recv_sem=recv_sem.at[me],
                device_id=device, device_id_type=MESH).start()

        target[me, live] = source[me, live]
        meanwhile()

        @pl.loop(1, devices)
        def finish(offset):
            other, device = peer(offset)
            pltpu.make_async_remote_copy(
                src_ref=source.at[other, live], dst_ref=target.at[other, live],
                send_sem=send_sem.at[other], recv_sem=recv_sem.at[other],
                device_id=device, device_id_type=MESH).wait()

    def outputs():
        for f in range(nspec):
            for x in range(cells_x):
                species_out[f, pl.ds(x * cells_y, cells_y)] = state[pl.ds(x * cells_y * SLOT + f, cells_y, stride=SLOT), :]
        for f in range(nflow - 1):
            flow_out[f] = moved[nspec + f]

    exchange(packed, spectra, out_send, out_recv, outputs)

    shape = spectra.shape
    flat = (shape[0] * shape[1], shape[2])
    value = dot_left(4, spectra[...].reshape(flat)).reshape(shape)
    turned = turn(value)
    re, im = tables[0], tables[1]
    a = value * re + turned * im
    b = turned * re - value * im
    value = dot_right(jnp.concatenate([a.reshape(flat), b.reshape(flat)], axis=1), 6).reshape(shape)

    kxy = tables[2]
    upper = lane < columns
    total = kxy * value
    total = total + pltpu.roll(total, columns, 2)
    crossed = pltpu.roll(value, columns, 2)
    even = pltpu.roll(jnp.where(upper, value, crossed), 4, 1)
    odd = pltpu.roll(jnp.where(upper, crossed, value), 6, 1)
    potential = (total + jnp.where(row < 2, even, odd)) * inverse[...]
    deep = jnp.where(upper, pltpu.roll(potential, 4, 1), pltpu.roll(potential, 2, 1))
    value = jnp.where(row < 4, kxy * potential, jnp.where(row < LIVE, deep, 0.0))

    turned = turn(value)
    value = dot_right(jnp.concatenate([value.reshape(flat), turned.reshape(flat)], axis=1), 8).reshape(shape)
    value = value * re - turn(value) * im
    unpacked[...] = dot_left(10, value.reshape(flat)).reshape(shape)
    exchange(unpacked, gathered, back_send, back_recv, lambda: None)
    gathered_out[...] = gathered[...]


def final_kernel(back_h, back_l, species_in, flow_in, gathered, species_hbm, flow_hbm, flow, sems):
    nflow, columns, depth = flow.shape
    store = pltpu.make_async_copy(species_in, species_hbm, sems.at[0])
    store.start()
    value = jnp.transpose(gathered[...].reshape(back_h.shape[0], 2 * columns))
    high, low = halves(value)
    a, b = back_h[...], back_l[...]
    result = mul(high, a) + mul(low, a) + mul(high, b)
    flow[0] = flow_in[0]
    flow[1] = flow_in[1] - result[:columns, :depth]
    flow[2] = flow_in[2] - result[columns:, :depth]
    flow[3] = flow_in[3] - (result[:columns, depth : 2 * depth] + result[columns:, 2 * depth :])
    flow[4] = flow_in[4]
    ship = pltpu.make_async_copy(flow, flow_hbm, sems.at[1])
    ship.start()
    store.wait()
    ship.wait()


def flame(
    species, flow_fields, classes, diffusivity, left_form, right_form, stoich, heat_release,
    arrhenius_prefactor, arrhenius_energy, newton_matrix, matrices, tables, back_h, back_l,
):
    grid_x, grid_y = lax.axis_size("gx"), lax.axis_size("gy")
    nspec, cells_x, cells_y, depth = species.shape
    nflow = flow_fields.shape[0]
    nfield = nspec + nflow
    nreac = left_form.shape[0]
    columns = cells_x * cells_y
    devices = grid_x * grid_y
    hbm = pl.BlockSpec(memory_space=pltpu.HBM)
    vmem = pl.BlockSpec(memory_space=pltpu.VMEM)
    dma = pltpu.SemaphoreType.DMA
    box = (devices, TILE, depth)
    shaped = lambda shape: jax.ShapeDtypeStruct(shape, F32)
    line = lambda a: a.reshape(1, -1)
    inputs = (
        species.reshape(nspec, columns, depth), flow_fields.reshape(nflow, columns, depth), classes, diffusivity,
        left_form.T, right_form.T, stoich.T, line(heat_release), line(arrhenius_prefactor), line(arrhenius_energy),
        newton_matrix, matrices, tables,
    )
    most = (max((cells_x - 2) * (cells_y - 2), columns) + 1) // 2
    scratch = [
        pltpu.VMEM((nfield, columns, depth), F32),
        pltpu.VMEM((nfield, columns, depth), F32),
        pltpu.VMEM((3, columns, depth), F32),
        pltpu.VMEM((2, nfield, cells_y, depth), F32),
        pltpu.VMEM((2, nfield, cells_x, depth), F32),
        pltpu.VMEM((2, nfield, cells_x, depth), F32),
        pltpu.VMEM((columns * SLOT, depth), F32),
        pltpu.VMEM((most, WAVES, 2 * depth), F32),
        pltpu.VMEM((most, ROWS, 2 * depth), F32),
        pltpu.VMEM((most, 3 * PIECE, 2 * depth), BF16),
        pltpu.VMEM((most, TILE, 2 * depth), F32),
        pltpu.SMEM(classes.shape, jnp.int32),
        pltpu.SMEM(diffusivity.shape, F32),
    ]
    scratch += [pltpu.VMEM(a.shape, F32) for a in inputs[4:11]]
    scratch += [
        pltpu.VMEM((depth, depth), F32),
        pltpu.VMEM((SLOT, depth), F32),
        pltpu.VMEM((ROWS, 2 * depth), F32),
        pltpu.VMEM(matrices.shape, BF16),
        pltpu.VMEM(tables.shape, F32),
    ]
    scratch += [pltpu.VMEM(box, F32)] * 5
    scratch += [dma((2,)), dma((9,)), dma((2,)), dma((4,)), dma((4,))] + [dma((devices,))] * 4
    species_done, flow_done, gathered = pl.pallas_call(
        functools.partial(flame_kernel, grid_x, grid_y),
        out_shape=(shaped((nspec, columns, depth)), shaped((nflow, columns, depth)), shaped(box)),
        in_specs=[hbm] * len(inputs),
        out_specs=(vmem, vmem, vmem),
        scratch_shapes=scratch,
        compiler_params=pltpu.CompilerParams(collective_id=0, has_side_effects=True, vmem_limit_bytes=FUSED_VMEM),
        name="flame",
    )(*[pltpu.with_memory_space_constraint(a, pltpu.HBM) for a in inputs])
    species_out, flow_out = pl.pallas_call(
        final_kernel,
        out_shape=(shaped((nspec, columns, depth)), shaped((nflow, columns, depth))),
        in_specs=[vmem] * 5,
        out_specs=(hbm, hbm),
        scratch_shapes=[pltpu.VMEM((nflow, columns, depth), F32), dma((2,))],
        compiler_params=pltpu.CompilerParams(vmem_limit_bytes=FINAL_VMEM),
        name="final",
    )(back_h, back_l, species_done, flow_done, gathered)
    return species_out.reshape(species.shape), flow_out.reshape(flow_fields.shape)


def solution(mesh):
    grid_x, grid_y = mesh.shape["gx"], mesh.shape["gy"]

    def step(species, flow_fields, classes, *rest):
        cells_x = species.shape[1] // grid_x
        cells_y = species.shape[2] // grid_y
        depth = species.shape[3]
        direct = (
            depth == 128 and cells_y == 8 and 2 * cells_x * cells_y == 128
            and depth == 4 * grid_x * grid_y
        )
        grids = (P(None, "gx", "gy", None), P(None, "gx", "gy", None), P("gx", "gy"))
        constants = ()
        if direct:
            constants = tuple(spectral_constants(grid_x, grid_y, cells_x, cells_y, depth))
        return jax.shard_map(
            flame if direct else shards,
            mesh=mesh,
            in_specs=grids + (P(),) * (len(rest) + len(constants)),
            out_specs=(P(None, "gx", "gy", None), P(None, "gx", "gy", None)),
            check_vma=False,
        )(species, flow_fields, classes, *rest, *constants)

    return step
```
